32 devices in a mesh: group: 2 (over y), expert: 4 (over z), req: 4 (over x, core).
Axes of the slice: x: 2, y: 2, z: 4, core: 2. Of those that a mesh axis runs over, the one named last changes fastest.
Arguments:
- verify_in: bfloat16 [128, 4096], P(('group', 'expert'), 'req'), parts along dimension 0, may hold values from -6 to 6
- expert_ids: int32 [128, 2], P(('group', 'expert')), parts along dimension 0, may hold values from 0 to 7, all different within a row; in each aligned block of 16 rows (0 to 15, 16 to 31, ...) at most 8 rows name the same one
- gate_weights: float32 [128, 2], P(('group', 'expert')), parts along dimension 0, may hold values from 0.2 to 1
- moe_gate: bfloat16 [32, 4096, 1792], P('expert', None, 'req'), may hold values from -0.09375 to 0.09375
- moe_up: bfloat16 [32, 4096, 1792], P('expert', None, 'req'), may hold values from -0.09375 to 0.09375
- moe_down: bfloat16 [32, 1792, 4096], P('expert', 'req'), may hold values from -0.09375 to 0.09375
- draft_emb: bfloat16 [2048, 4096], P(('group', 'req'), 'expert'), parts along dimension 0, may hold values from -6 to 6
- draft_feat: bfloat16 [2048, 4096], P(('group', 'req'), 'expert'), parts along dimension 0, may hold values from -18 to 18
- parents: int32 [2048], P(('group', 'req')), parts along dimension 0, may hold values from 0 to 1023, as said below
- join_weight: bfloat16 [8192, 4096], P('req', 'expert'), may hold values from -3 to 3
- norm_gain: float32 [4096], P('expert'), may hold values from 0.5 to 1.5
- draft_gate: bfloat16 [4096, 7168], P('req', 'expert'), may hold values from -0.09375 to 0.09375
- draft_up: bfloat16 [4096, 7168], P('req', 'expert'), may hold values from -0.09375 to 0.09375
- draft_down: bfloat16 [7168, 4096], P('expert', 'req'), may hold values from -0.09375 to 0.09375
Outputs:
- verify_out: bfloat16 [128, 4096], P(('group', 'expert'), 'req'), parts along dimension 0
- draft_out: bfloat16 [2048, 4096], P(('group', 'req'), 'expert'), parts along dimension 0
The draws below stay inside these ranges and needn't reach their ends.
There are 2 independent parts, one for each index of `group`. The reference program is written for one: setup_inputs(seed, part) draws one part's arguments, and reference() takes and returns one part's arrays. A program takes and returns all parts, laid end to end along the dimension named above; an argument that names none is the same for every part. Nothing has to cross between parts.
Inputs may be any that keep to these rules, and one draw needn't show every extreme that they name: `expert_ids`: each row names two different experts; within the rows of one index of expert, no expert is named more than 8 times. `parents`: each row's parent is a row of the same tree of 64 consecutive rows at an earlier position; a tree's first row is its own parent.
All inputs are finite; a program needn't handle non-finite values.
Results may differ from the reference program's by a relative error of at most 0.015.
Values may be sent and summed in bfloat16 or wider, within the bound.
No kernel may reach another device: no remote copies, remote signals or barrier semaphores. Data moves between devices by JAX's collectives and lax.ppermute only.
A program may use at most 256 MiB of HBM per device.

```python
import math
import jax
import jax.numpy as jnp
import numpy as np
from jax import lax

D = 4096
EXPERTS = 8
FF = 7168
DFF = 7168
SLICES = 4
TREE = 64
VROW_DEV = 16
CAP = 8
VROWS = 64
DROWS = 1024
N_EXPERT = 4
N_REQ = 4


def draw_draft_feat(key, part):
    base_key, scale_key = jax.random.split(jax.random.fold_in(key, 11), 2)
    base = jnp.clip(jax.random.normal(base_key, (DROWS, D), jnp.float32), -6.0, 6.0)
    scales = jnp.exp(jax.random.uniform(scale_key, (DROWS, 1), jnp.float32, math.log(0.3), math.log(3.0)))
    return (base * scales).astype(jnp.bfloat16)


def draw_join_weight(key, part):
    base_key, jitter_key = jax.random.split(jax.random.fold_in(key, 23), 2)
    positions = jnp.arange(D, dtype=jnp.float32) / D
    rising = jnp.exp(math.log(3.0) * (positions - 0.5))[None, :]
    jitter = jnp.exp(jax.random.uniform(jitter_key, (1, D), jnp.float32, -1.15, 1.15))
    column_scale = rising * jitter / math.sqrt(2.0 * D)
    base = jnp.clip(jax.random.normal(base_key, (2 * D, D), jnp.float32), -6.0, 6.0)
    return (base * column_scale).astype(jnp.bfloat16)


def draw_parents(key, part):
    position = jnp.arange(DROWS, dtype=jnp.int32)
    within = position % TREE
    offsets = jax.random.randint(jax.random.fold_in(key, 7), (DROWS,), 0, jnp.maximum(within, 1), jnp.int32)
    return (position - within + offsets).astype(jnp.int32)


def raised(array, stream_key, source, target, shards_of, factor):
    def block_of(dim):
        return (jnp.arange(array.shape[dim]) // (array.shape[dim] // shards_of)).reshape((-1,) + (1,) * (array.ndim - 1 - dim))

    first = jax.random.permutation(stream_key, shards_of)[block_of(target)]
    other_side = (block_of(target) + shards_of // 2) % shards_of
    return jnp.where((block_of(source) == first) | (block_of(source) == other_side), factor * array, array)


def level_of(rng, extent, shards, smallest, largest):
    gain, own = 1.0, jax.random.fold_in(rng, 6)
    for dim, blocks in shards:
        draws = jnp.exp(jax.random.uniform(jax.random.fold_in(own, dim), (blocks,), jnp.float32, smallest / len(shards), largest / len(shards)))
        gain = gain * jnp.repeat(draws, extent[dim] // blocks).reshape([-1 if axis == dim else 1 for axis in range(len(extent))])
    return gain


def deal_out(stream_key, own, number, rows, amount, top, bound, lean):
    sequence = jax.random.permutation(stream_key, amount)
    heavy_load, ordinary = portions_of(amount, rows * top, bound, lean, True), portions_of(amount, rows * top, bound, lean, False)
    places = jnp.arange(amount)

    def named(sizes, offset_by):
        used = int((sizes > 0).sum())
        fixed = max(1, used // 4)
        moved = fixed + (places - fixed + offset_by * (used - fixed)) % max(1, amount - fixed)
        return jnp.zeros((amount,), jnp.int32).at[sequence[jnp.where(places < fixed, places, moved)]].set(jnp.asarray(sizes, jnp.int32))

    sizes = jnp.where(number % 4 == 0, named(heavy_load, number // 4), named(ordinary, number - number // 4 - 1))
    mixed = jax.random.permutation(jax.random.fold_in(own, 3), amount)
    giver, receiver = mixed[0:amount // 2 * 2:2], mixed[1:amount // 2 * 2:2]
    slack = jnp.minimum(sizes[giver] - 1, bound - sizes[receiver]) // 2
    slack = jnp.where((giver == sequence[0]) | (receiver == sequence[0]) | (sizes[receiver] == 0), 0, jnp.maximum(slack, 0))
    moved = jax.random.randint(jax.random.fold_in(own, 4), (amount // 2,), 0, 1 << 20) % (slack + 1)
    sizes = sizes.at[giver].add(-moved).at[receiver].add(moved)
    items = jnp.searchsorted(jnp.cumsum(sizes), jnp.arange(rows * top), side="right").astype(jnp.int32)
    grid = items.reshape(top, rows).T
    grid = grid[jax.random.permutation(jax.random.fold_in(own, 1), rows)]
    offset_by = jax.random.randint(jax.random.fold_in(own, 2), (rows, 1), 0, top)
    return jnp.take_along_axis(grid, (jnp.arange(top)[None, :] + offset_by) % top, axis=1)


def portions_of(count, total, bound, skew, full):
    weights = [(1 << 20) // math.isqrt(grade ** skew) + 1 for grade in range(1, count + 1)]
    largest = bound if full else min(bound, max(-(-total // count), total * weights[0] // sum(weights)))
    least = 1 if total - largest >= count - 1 else 0
    given, spare = [largest] + [least] * (count - 1), total - largest - least * (count - 1)
    while spare > 0:
        free = [i for i in range(1, count) if given[i] < largest] or [i for i in range(1, count) if given[i] < bound]
        pool, left = sum([weights[i] for i in free]), spare
        for i in free:
            extra = min(bound - given[i], max(1, left * weights[i] // pool), spare)
            given[i] = given[i] + extra
            spare = spare - extra
    return np.array(given)


def noise(rng, dims, width, bound, cuts=(), kind=jnp.bfloat16):
    factor_of = level_of(rng, dims, cuts, -0.22, 0.18) if cuts else 1.0
    drawn = jax.random.normal(rng, dims, jnp.float32) * width * factor_of
    return jnp.minimum(jnp.maximum(drawn, -bound), bound).astype(kind)


def heavy_noise(key, extent, spread, most, cuts, heavy, held_as=jnp.bfloat16):
    entries = spread * jax.random.normal(key, extent, jnp.float32)
    if cuts:
        entries = entries * level_of(key, extent, cuts, -0.22, 0.18)
    return jnp.clip(raised(entries, jax.random.fold_in(key, 3), *heavy), -most, most).astype(held_as)


def setup_inputs(seed: int = 0, part: int = 0) -> dict:
    seeds = jax.random.split(jax.random.key(seed), 15)
    part_keys = jax.random.split(jax.random.fold_in(seeds[14], part), 15)
    verify_in = noise(part_keys[0], (VROWS, D), 1.0, 6.0, ((0, 4), (1, 4)))
    expert_ids_keys = jax.random.split(jax.random.fold_in(part_keys[1], 1), VROWS // VROW_DEV)
    expert_ids_turns = jax.random.permutation(jax.random.fold_in(part_keys[1], 3), VROWS // VROW_DEV)
    expert_ids = jax.vmap(lambda own, number: deal_out(jax.random.fold_in(part_keys[1], 2), own, number, VROW_DEV, EXPERTS, 2, CAP, 2))(expert_ids_keys, expert_ids_turns).reshape((VROWS, 2))
    gate_weights = jnp.clip(0.2 + 0.8 * jax.random.uniform(part_keys[2], (VROWS, 2), jnp.float32) ** level_of(part_keys[2], (VROWS, 2), ((0, 4),), -0.2, 0.2), 0.2, 1.0)
    moe_gate = noise(seeds[3], (EXPERTS * SLICES, D, FF // SLICES), D ** -0.5, 0.09375, ((0, 4), (2, 4)))
    moe_up = noise(seeds[4], (EXPERTS * SLICES, D, FF // SLICES), D ** -0.5, 0.09375, ((0, 4), (2, 4)))
    moe_down = heavy_noise(seeds[5], (EXPERTS * SLICES, FF // SLICES, D), FF ** -0.5, 0.09375, ((0, 4), (1, 4)), (1, 2, 4, 2.0))
    draft_emb = noise(part_keys[6], (DROWS, D), 1.0, 6.0, ((0, 4), (1, 4)))
    draft_feat = draw_draft_feat(jax.random.fold_in(jax.random.fold_in(seeds[14], part), 71), part)
    parents = draw_parents(jax.random.fold_in(jax.random.fold_in(seeds[14], part), 71), part)
    join_weight = draw_join_weight(jax.random.fold_in(seeds[14], 71), part)
    norm_gain = jnp.clip(1.0 + 0.1 * jax.random.normal(seeds[10], (D,), jnp.float32), 0.5, 1.5)
    draft_gate = noise(seeds[11], (D, DFF), D ** -0.5, 0.09375, ((0, 4), (1, 4)))
    draft_up = noise(seeds[12], (D, DFF), D ** -0.5, 0.09375, ((0, 4), (1, 4)))
    draft_down = heavy_noise(seeds[13], (DFF, D), DFF ** -0.5, 0.09375, ((0, 4), (1, 4)), (0, 1, 4, 2.0))
    return dict(verify_in=verify_in, expert_ids=expert_ids, gate_weights=gate_weights, moe_gate=moe_gate, moe_up=moe_up, moe_down=moe_down, draft_emb=draft_emb, draft_feat=draft_feat, parents=parents, join_weight=join_weight, norm_gain=norm_gain, draft_gate=draft_gate, draft_up=draft_up, draft_down=draft_down)


def slot_numbers(expert_ids):
    blocks = expert_ids.reshape(N_EXPERT, VROW_DEV * 2)
    onehot = (blocks[:, :, None] == jnp.arange(EXPERTS, dtype=jnp.int32)[None, None, :]).astype(jnp.int32)
    before = jnp.cumsum(onehot, axis=1) - onehot
    return lax.optimization_barrier(jnp.sum(before * onehot, axis=2)).reshape(VROWS, 2).astype(jnp.int32)

def verify_layer(verify_in, expert_ids, gate_weights, moe_gate, moe_up, moe_down):
    slot_index = slot_numbers(expert_ids)
    row_ids = jnp.arange(VROWS, dtype=jnp.int32)
    position = ((row_ids // VROW_DEV)[:, None] * CAP + slot_index).astype(jnp.int32)
    table = jnp.full((EXPERTS, N_EXPERT * CAP), VROWS, jnp.int32)
    table = table.at[expert_ids, position].set(jnp.broadcast_to(row_ids[:, None], (VROWS, 2)).astype(jnp.int32))
    padded = jnp.concatenate([verify_in, jnp.zeros((1, D), jnp.bfloat16)], axis=0)
    slice_width = FF // SLICES
    pieces = SLICES * N_REQ
    piece_width = FF // pieces

    def one_expert(inputs):
        chosen_rows, gate_w, up_w, down_w = inputs
        chosen = padded[chosen_rows]
        gate_full = jnp.transpose(gate_w, (1, 0, 2)).reshape(D, FF)
        up_full = jnp.transpose(up_w, (1, 0, 2)).reshape(D, FF)
        gate_sum = jnp.dot(chosen, gate_full, preferred_element_type=jnp.float32)
        up_sum = jnp.dot(chosen, up_full, preferred_element_type=jnp.float32)
        hidden = (jax.nn.silu(gate_sum) * up_sum).astype(jnp.bfloat16)
        hidden_parts = hidden.reshape(hidden.shape[0], pieces, piece_width).astype(jnp.float32)
        down_parts = down_w.reshape(pieces, piece_width, D).astype(jnp.float32)
        partial_value = jnp.einsum('mpq,pqd->pmd', hidden_parts, down_parts)
        rounded = lax.optimization_barrier(partial_value.astype(jnp.bfloat16))
        result = lax.optimization_barrier(jnp.sum(rounded.astype(jnp.float32), axis=0))
        return result.astype(jnp.bfloat16)
    outputs = lax.map(one_expert, (table, moe_gate.reshape(EXPERTS, SLICES, D, slice_width), moe_up.reshape(EXPERTS, SLICES, D, slice_width), moe_down.reshape(EXPERTS, SLICES, slice_width, D)))
    picked = outputs[expert_ids, position].astype(jnp.float32)
    return lax.optimization_barrier(jnp.sum(gate_weights[:, :, None] * picked, axis=1)).astype(jnp.bfloat16)

def draft_step(draft_emb, draft_feat, parents, join_weight, norm_gain, draft_gate, draft_up, draft_down):
    joined = jnp.concatenate([draft_emb, draft_feat[parents]], axis=1)
    joined_state = jnp.dot(joined, join_weight, preferred_element_type=jnp.float32)
    meansq = lax.optimization_barrier(jnp.mean(joined_state * joined_state, axis=1, keepdims=True))
    normed = (joined_state * lax.rsqrt(meansq + 1e-05) * norm_gain[None, :]).astype(jnp.bfloat16)
    gate_sum = jnp.dot(normed, draft_gate, preferred_element_type=jnp.float32)
    up_sum = jnp.dot(normed, draft_up, preferred_element_type=jnp.float32)
    hidden = (jax.nn.silu(gate_sum) * up_sum).astype(jnp.bfloat16)
    mlp_sum = jnp.dot(hidden, draft_down, preferred_element_type=jnp.float32)
    return (joined_state + mlp_sum).astype(jnp.bfloat16)

def reference(verify_in, expert_ids, gate_weights, moe_gate, moe_up, moe_down, draft_emb, draft_feat, parents, join_weight, norm_gain, draft_gate, draft_up, draft_down):
    verify_out = verify_layer(verify_in, expert_ids, gate_weights, moe_gate, moe_up, moe_down)
    draft_out = draft_step(draft_emb, draft_feat, parents, join_weight, norm_gain, draft_gate, draft_up, draft_down)
    return (verify_out, draft_out)
```

```python
import jax
import jax.numpy as jnp
from jax import lax
from jax.sharding import PartitionSpec as P

EXPERTS = 8
EPS = 1e-05


F32 = jnp.float32
BF16 = jnp.bfloat16


def matmul(a, b):
    return jnp.dot(a, b, preferred_element_type=F32)


class Device:
    def __init__(self, mesh):
        self.n_g, self.n_e, self.n_r = (mesh.shape[a] for a in ("group", "expert", "req"))
        self.half = self.n_r // 2

    def enter(self):
        self.g = lax.axis_index("group")
        self.e = lax.axis_index("expert")
        self.r = lax.axis_index("req")
        self.hi = self.r // self.half
        self.lo = self.r % self.half

    def far(self, a):
        n, h = self.n_r, self.half
        return lax.ppermute(a, "req", [(i, (i + h) % n) for i in range(n)])

    def near(self, a):
        return lax.ppermute(a, "req", [(i, i ^ 1) for i in range(self.n_r)])

    def other_group(self, a):
        return lax.ppermute(a, "group", [(0, 1), (1, 0)])

    def shift(self, a, j):
        n = self.n_e
        return lax.ppermute(a, "expert", [(i, (i + j) % n) for i in range(n)])

    def line_gather(self, a):
        one = lax.ppermute(a, "expert", [(0, 1), (1, 2), (2, 3)])
        back = lax.ppermute(a, "expert", [(1, 0), (2, 1), (3, 2)])
        two = self.shift(a, 2)
        relay = lax.ppermute(two, "expert", [(2, 3), (1, 0)])
        return [a, jnp.where(self.e == 0, relay, one), two, jnp.where(self.e == 3, relay, back)]

    def source(self, j):
        return (self.e - j) % self.n_e


def split3(v):
    hi = v.astype(BF16)
    rest = v - hi.astype(F32)
    mid = rest.astype(BF16)
    low = (rest - mid.astype(F32)).astype(BF16)
    return [hi, mid, low]


def columns(a, start, width):
    return lax.dynamic_slice_in_dim(a, start, width, axis=1)


def rows(a, start, count):
    return lax.dynamic_slice_in_dim(a, start, count, axis=0)


def verify_layer(dev, verify_in, expert_ids, gate_weights, moe_gate, moe_up, moe_down):
    n_row, width = verify_in.shape
    n_k, d_model, n_f = moe_gate.shape
    top = expert_ids.shape[1]
    per_expert = n_k * dev.n_e // EXPERTS
    row_all = lax.all_gather(verify_in, "req", axis=1, tiled=True)
    extra = [expert_ids.astype(BF16)] + split3(gate_weights)
    extra = jnp.concatenate(extra + [jnp.zeros((n_row, 128 - 4 * top), BF16)], axis=1)
    packed = jnp.concatenate([row_all, extra], axis=1)
    packed = jnp.concatenate([packed] + [dev.shift(packed, j) for j in range(1, dev.n_e)], axis=0)
    x = packed[:, :d_model]
    ids, w_hi, w_mid, w_low = (packed[:, d_model + i * top : d_model + (i + 1) * top].astype(F32) for i in range(4))
    weight = w_hi + w_mid + w_low
    local = (dev.e * n_k + jnp.arange(n_k)) // per_expert
    coef = jnp.sum(weight[None] * (ids[None] == local[:, None, None].astype(F32)), axis=2)
    gate = jnp.einsum("md,kdf->kmf", x, moe_gate, preferred_element_type=F32)
    up = jnp.einsum("md,kdf->kmf", x, moe_up, preferred_element_type=F32)
    hidden = (jax.nn.silu(gate) * up * coef[:, :, None]).astype(BF16)
    part = jnp.einsum("kmf,kfd->md", hidden, moe_down, preferred_element_type=F32)
    part = part.reshape(part.shape[0], 2, dev.half, width)
    mine = lax.dynamic_index_in_dim(part, dev.lo, axis=2, keepdims=False)
    given = lax.dynamic_index_in_dim(part, 1 - dev.lo, axis=2, keepdims=False)
    mine = mine + dev.near(given.astype(BF16).reshape(-1, 2 * width)).astype(F32).reshape(-1, 2, width)
    given = lax.dynamic_index_in_dim(mine, 1 - dev.hi, axis=1, keepdims=False)
    mine = lax.dynamic_index_in_dim(mine, dev.hi, axis=1, keepdims=False)
    mine = mine + dev.far(given.astype(BF16)).astype(F32)
    mine = mine.reshape(dev.n_e, n_row, width)
    out = mine[0]
    for j in range(1, dev.n_e):
        out = out + dev.shift(mine[j].astype(BF16), dev.n_e - j).astype(F32)
    return out.astype(BF16)


def fetch(dev, weight):
    count = weight.shape[0] // dev.n_g
    first = dev.g * count
    far = dev.far(rows(weight, first, count))
    pieces = [(0, 0, weight), (2, first, far)]
    if dev.n_g == 2:
        pieces.append((2, count - first, dev.other_group(far)))
    return pieces + [(block ^ 1, start, dev.near(piece)) for block, start, piece in pieces]


def draft_step(dev, draft_emb, draft_feat, parents, join_weight, norm_gain, draft_gate, draft_up, draft_down):
    n_row, width = draft_emb.shape
    d_model = width * dev.n_e
    placing = (parents[:, None] - dev.r * n_row == jnp.arange(n_row)[None, :]).astype(BF16)
    feat = matmul(placing, draft_feat).astype(BF16)
    first = dev.hi == 0
    own = jnp.where(first, draft_emb, feat)
    given = jnp.where(first, feat, draft_emb)
    taken = dev.far(given)

    join_near = dev.near(join_weight)
    is_low = dev.lo == 0
    join_full = jnp.concatenate(
        [jnp.where(is_low, join_weight, join_near), jnp.where(is_low, join_near, join_weight)], axis=0
    )

    if dev.n_e == 4:
        own_all = dev.line_gather(own)
        taken_all = dev.line_gather(taken)
        state = jnp.zeros((n_row, width), F32)
        other = jnp.zeros((n_row, width), F32)
        for j in range(dev.n_e):
            block = rows(join_full, dev.source(j) * width, width)
            other = other + matmul(taken_all[j], block)
            state = state + matmul(own_all[j], block)
    else:
        state = matmul(lax.all_gather(own, "expert", axis=1, tiled=True), join_full)
        other = matmul(lax.all_gather(taken, "expert", axis=1, tiled=True), join_full)
    joined_state = state + dev.far(other.astype(BF16)).astype(F32)

    scaled = (joined_state * norm_gain[None, :]).astype(BF16)
    if dev.n_e == 4:
        inverse = 1.0 / norm_gain
        inverses = [inverse] + [dev.shift(inverse, j) for j in range(1, dev.n_e)]
        chunks = dev.line_gather(scaled)
        full = jnp.zeros((n_row, d_model), BF16)
        squares = jnp.zeros((n_row,), F32)
        for j in range(dev.n_e):
            full = lax.dynamic_update_slice_in_dim(full, chunks[j], dev.source(j) * width, axis=1)
            back = chunks[j].astype(F32) * inverses[j][None, :]
            squares = squares + jnp.sum(back * back, axis=1)
    else:
        full = lax.all_gather(scaled, "expert", axis=1, tiled=True)
        squares = lax.psum(jnp.sum(joined_state * joined_state, axis=1), "expert")
    row_scale = lax.rsqrt(squares / d_model + EPS)[:, None]

    inner = draft_gate.shape[0]

    def product(pieces):
        total = 0.0
        for block, start, piece in pieces:
            total = total + matmul(columns(full, (dev.r ^ block) * inner + start, piece.shape[0]), piece)
        return total

    gate = product(fetch(dev, draft_gate)) * row_scale
    up = product(fetch(dev, draft_up)) * row_scale
    hidden = (jax.nn.silu(gate) * up).astype(BF16)

    out_width = draft_down.shape[1]
    blocks = [0.0] * dev.n_r
    for block, start, piece in fetch(dev, draft_down):
        blocks[block] = blocks[block] + matmul(columns(hidden, start, piece.shape[0]), piece)
    terms = jnp.zeros((n_row, d_model), BF16)
    for block in range(dev.n_r):
        terms = lax.dynamic_update_slice_in_dim(terms, blocks[block].astype(BF16), (dev.r ^ block) * out_width, axis=1)
    if dev.n_e == 4:
        total = columns(terms, dev.e * width, width).astype(F32)
        for j in range(1, dev.n_e):
            total = total + dev.shift(columns(terms, (dev.e + j) % dev.n_e * width, width), j).astype(F32)
    else:
        total = lax.psum_scatter(terms, "expert", scatter_dimension=1, tiled=True).astype(F32)
    return (joined_state + total).astype(BF16)


def solution(mesh):
    dev = Device(mesh)

    def per_device(
        verify_in, expert_ids, gate_weights, moe_gate, moe_up, moe_down,
        draft_emb, draft_feat, parents, join_weight, norm_gain, draft_gate, draft_up, draft_down,
    ):
        dev.enter()
        verify_out = verify_layer(dev, verify_in, expert_ids, gate_weights, moe_gate, moe_up, moe_down)
        draft_out = draft_step(
            dev, draft_emb, draft_feat, parents, join_weight, norm_gain, draft_gate, draft_up, draft_down
        )
        return (verify_out, draft_out)

    in_specs = (
        P(("group", "expert"), "req"),
        P(("group", "expert"), None),
        P(("group", "expert"), None),
        P("expert", None, "req"),
        P("expert", None, "req"),
        P("expert", "req", None),
        P(("group", "req"), "expert"),
        P(("group", "req"), "expert"),
        P(("group", "req")),
        P("req", "expert"),
        P("expert"),
        P("req", "expert"),
        P("req", "expert"),
        P("expert", "req"),
    )
    out_specs = (P(("group", "expert"), "req"), P(("group", "req"), "expert"))
    return jax.shard_map(
        per_device, mesh=mesh, in_specs=in_specs, out_specs=out_specs, check_vma=False
    )
```
